512 devices in a mesh: groups: 2 (over y), sp: 32 (over z), tp: 4 (over x), dp: 2 (over core).
Axes of the slice: x: 4, y: 2, z: 32, core: 2. Of those that a mesh axis runs over, the one named last changes fastest.
The devices are a block of a 4x8x32 slice.
Arguments:
- queries: bfloat16 [65536, 4096], P(('groups', 'tp', 'dp', 'sp')), parts along dimension 0, may hold values from -6 to 6
- keys: bfloat16 [65536, 512], P(('groups', 'tp', 'dp', 'sp')), parts along dimension 0, may hold values from -6 to 6
- values: bfloat16 [65536, 512], P(('groups', 'tp', 'dp', 'sp')), parts along dimension 0, may hold values from -6 to 6
- doc_lengths: int32 [64], P('groups'), parts along dimension 0, may hold values from 1 to 2048, 32768 in all
Outputs:
- attended: bfloat16 [65536, 4096], P(('groups', 'tp', 'dp', 'sp')), parts along dimension 0
The draws below stay inside these ranges and needn't reach their ends.
There are 2 independent parts, one for each index of `groups`. The reference program is written for one: setup_inputs(seed, part) draws one part's arguments, and reference() takes and returns one part's arrays. A program takes and returns all parts, laid end to end along the dimension named above; each array names one. Nothing has to cross between parts.
Inputs may be any that keep to these rules, and one draw needn't show every extreme that they name: `doc_lengths`: 32 documents whose lengths sum to 32768; the longest has exactly 2048 tokens.
All inputs are finite; a program needn't handle non-finite values.
Results may differ from the reference program's by a relative error of at most 0.0038.
Values may be sent and summed in bfloat16 or wider, within the bound.
No kernel may reach another device: no remote copies, remote signals or barrier semaphores. Data moves between devices by JAX's collectives and lax.ppermute only.
A program may use at most 64 MiB of HBM per device.

```python
import math
import jax
import jax.numpy as jnp
import numpy as np
from jax import lax

QUERY_HEADS = 32
KEY_VALUE_HEADS = 4
HEAD_SIZE = 128
SEQUENCE_TOKENS = 32768
LONGEST_DOCUMENT = 2048
NDOC = 32


def draw_keys(key, part):
    attention_output = jnp.clip(jax.random.normal(jax.random.fold_in(key, 11), (SEQUENCE_TOKENS, KEY_VALUE_HEADS * HEAD_SIZE), jnp.float32), -6.0, 6.0)
    return attention_output.astype(jnp.bfloat16)


def draw_queries(key, part):
    attention_output = jnp.clip(jax.random.normal(jax.random.fold_in(key, 13), (SEQUENCE_TOKENS, QUERY_HEADS * HEAD_SIZE), jnp.float32), -6.0, 6.0)
    return attention_output.astype(jnp.bfloat16)


def block_levels(key, shape, pieces, smallest, top_value):
    level = 1.0
    for position, parts in pieces:
        heights = jax.random.uniform(jax.random.fold_in(jax.random.fold_in(key, 6), position), (parts,), jnp.float32, smallest / len(pieces), top_value / len(pieces))
        level = level * jnp.repeat(jnp.exp(heights), shape[position] // parts).reshape((-1,) + (1,) * (len(shape) - 1 - position))
    return level


def profile(amount, total, most, slope):
    loads = [(1 << 20) // math.isqrt(grade ** slope) + 1 for grade in range(2, amount + 1)]
    rest, given = total - most - (amount - 1), [1] * (amount - 1)
    while rest > 0:
        free = [i for i in range(amount - 1) if given[i] < most]
        whole, left = sum([loads[i] for i in free]), rest
        for i in free:
            extra = min(most - given[i], max(1, left * loads[i] // whole), rest)
            given[i] = given[i] + extra
            rest = rest - extra
    return np.array([most] + given)


def uneven(key, count, total, most, slope):
    if count == 2:
        one = jax.random.randint(key, (), max(1, total - most), min(most, total - 1) + 1)
        return jnp.stack([one, total - one])
    tallies = jnp.asarray(profile(count, total, most, slope), jnp.int32)
    couples = (count - 1) // 2
    source_of, sink = tallies[1:1 + 2 * couples:2], tallies[2:2 + 2 * couples:2]
    margin = jnp.minimum(source_of - 1, most - sink)
    moved = jax.random.randint(jax.random.fold_in(key, 1), (couples,), 0, 1 << 20) % (margin + 1)
    tallies = tallies.at[1:1 + 2 * couples:2].set(source_of - moved).at[2:2 + 2 * couples:2].set(sink + moved)
    return tallies[jax.random.permutation(jax.random.fold_in(key, 2), count)]


def centred(stream_key, extent, spread, bound, shards=(), kind=jnp.bfloat16):
    array = jax.random.normal(stream_key, extent, jnp.float32) * spread
    if len(shards) > 0:
        array = block_levels(stream_key, extent, shards, -0.22, 0.18) * array
    return jnp.clip(array, min=-bound, max=bound).astype(kind)


def setup_inputs(seed: int = 0, part: int = 0) -> dict:
    key_list = jax.random.split(jax.random.key(seed), 5)
    part_splits = jax.random.split(jax.random.fold_in(key_list[4], part), 5)
    return {
        "queries": draw_queries(jax.random.fold_in(jax.random.fold_in(key_list[4], part), 71), part),
        "keys": draw_keys(jax.random.fold_in(jax.random.fold_in(key_list[4], part), 71), part),
        "values": centred(part_splits[2], (SEQUENCE_TOKENS, KEY_VALUE_HEADS * HEAD_SIZE), 1.0, 6.0, ((0, 256),)),
        "doc_lengths": uneven(part_splits[3], NDOC, SEQUENCE_TOKENS, LONGEST_DOCUMENT, 2).astype(jnp.int32),
    }


def reference(queries, keys, values, doc_lengths):
    ends = jnp.cumsum(doc_lengths).astype(jnp.int32)
    positions = jnp.arange(SEQUENCE_TOKENS, dtype=jnp.int32)
    doc = jnp.sum((positions[:, None] >= ends[None, :]).astype(jnp.int32), axis=1)
    query_group = QUERY_HEADS // KEY_VALUE_HEADS
    block = math.gcd(LONGEST_DOCUMENT, 512)
    blocks = SEQUENCE_TOKENS // block
    reach = LONGEST_DOCUMENT + block
    q_heads = queries.reshape(SEQUENCE_TOKENS, QUERY_HEADS, HEAD_SIZE).transpose(1, 0, 2)
    leading_part = jnp.zeros((LONGEST_DOCUMENT, KEY_VALUE_HEADS * HEAD_SIZE), jnp.bfloat16)
    key_head_rows = jnp.concatenate([leading_part, keys], axis=0).reshape(SEQUENCE_TOKENS + LONGEST_DOCUMENT, KEY_VALUE_HEADS, HEAD_SIZE).transpose(1, 0, 2)
    value_head_rows = jnp.concatenate([leading_part, values], axis=0).reshape(SEQUENCE_TOKENS + LONGEST_DOCUMENT, KEY_VALUE_HEADS, HEAD_SIZE).transpose(1, 0, 2)
    pad_pos = jnp.arange(SEQUENCE_TOKENS + LONGEST_DOCUMENT, dtype=jnp.int32) - LONGEST_DOCUMENT
    pad_doc = jnp.concatenate([jnp.full((LONGEST_DOCUMENT,), -1, jnp.int32), doc.astype(jnp.int32)], axis=0)
    scale = HEAD_SIZE ** -0.5

    def one_head(head):
        q_all = lax.dynamic_index_in_dim(q_heads, head, 0, keepdims=False)
        k_all = lax.dynamic_index_in_dim(key_head_rows, head // query_group, 0, keepdims=False)
        v_all = lax.dynamic_index_in_dim(value_head_rows, head // query_group, 0, keepdims=False)

        def one_block(index):
            first = (index * block).astype(jnp.int32)
            q_rows = lax.dynamic_slice_in_dim(q_all, first, block, 0)
            q_pos = first + jnp.arange(block, dtype=jnp.int32)
            q_doc = lax.dynamic_slice_in_dim(doc, first, block, 0)
            k_rows = lax.dynamic_slice_in_dim(k_all, first, reach, 0)
            v_rows = lax.dynamic_slice_in_dim(v_all, first, reach, 0)
            k_pos = lax.dynamic_slice_in_dim(pad_pos, first, reach, 0)
            k_doc = lax.dynamic_slice_in_dim(pad_doc, first, reach, 0)
            score = jnp.dot(q_rows, k_rows.T, preferred_element_type=jnp.float32) * scale
            live = (k_pos[None, :] <= q_pos[:, None]) & (k_doc[None, :] == q_doc[:, None])
            top = jnp.max(jnp.where(live, score, -jnp.inf), axis=1)
            weight = jnp.where(live, jnp.exp(score - top[:, None]), 0.0)
            total = jnp.sum(weight, axis=1)
            summed = jnp.dot(weight.astype(jnp.bfloat16), v_rows, preferred_element_type=jnp.float32)
            return (summed / total[:, None]).astype(jnp.bfloat16)

        return lax.map(one_block, jnp.arange(blocks, dtype=jnp.int32)).reshape(SEQUENCE_TOKENS, HEAD_SIZE)

    attention_output = lax.map(one_head, jnp.arange(QUERY_HEADS, dtype=jnp.int32))
    return attention_output.transpose(1, 0, 2).reshape(SEQUENCE_TOKENS, QUERY_HEADS * HEAD_SIZE)
```

```python
import functools
import math

import jax
import jax.numpy as jnp
from jax import lax
from jax.experimental import pallas as pl
from jax.experimental.pallas import tpu as pltpu
from jax.sharding import PartitionSpec as P

HEAD_SIZE = 128
LONGEST = 2048
TEAM = 4
TILE = 128
DEAD = -1e30


def shift(block, distance):
    names = ("sp", "tp", "dp")
    sp, tp, dp = (lax.axis_size(name) for name in names)
    count = sp * tp * dp

    def flat(place):
        token_range, within = divmod(place % count, sp)
        return within * tp * dp + token_range

    route = [(flat(i), flat(i + distance)) for i in range(count)]
    return lax.ppermute(block, names, route)


def attend_kernel(first_ref, low_ref, q_ref, own_ref, *refs, back, split, heads):
    ahead, behind = refs[:back], refs[back : 2 * back]
    o_ref, kv_ref, m_ref, l_ref, acc_ref = refs[2 * back :]
    span = own_ref.shape[0]
    factor = HEAD_SIZE ** (-0.5) * math.log2(math.e)
    for place in range(back):
        kv_ref[place, :split] = ahead[back - 1 - place][...]
        kv_ref[place, split:] = behind[back - 1 - place][...]
    kv_ref[back] = own_ref[...]
    pair_rows = 2 * TILE

    def one_tile(tile, _):
        rows = pl.ds(pl.multiple_of(tile * TILE, TILE), TILE)
        m_ref[...] = jnp.full_like(m_ref, DEAD)
        l_ref[...] = jnp.zeros_like(l_ref)
        acc_ref[...] = jnp.zeros_like(acc_ref)
        low = low_ref[rows, :]

        def one_span(place, _):
            key = place * span + lax.broadcasted_iota(jnp.int32, (TILE, span), 1)
            mine = back * span + tile * TILE + lax.broadcasted_iota(jnp.int32, (TILE, span), 0)
            bias = jnp.where((key >= low) & (key <= mine), 0.0, DEAD)
            bias = jnp.concatenate([bias, bias], axis=0)
            k = kv_ref[place, :, :HEAD_SIZE]
            v = kv_ref[place, :, HEAD_SIZE:]
            for pair in range(heads // 2):
                at = pl.ds(pair * pair_rows, pair_rows)
                q = jnp.concatenate(
                    [
                        q_ref[rows, (2 * pair + i) * HEAD_SIZE : (2 * pair + i + 1) * HEAD_SIZE]
                        for i in range(2)
                    ],
                    axis=0,
                )
                score = lax.dot_general(q, k, (((1,), (1,)), ((), ())), preferred_element_type=jnp.float32)
                score = score + bias
                old = m_ref[at, :1]
                top = jnp.maximum(old, jnp.max(score, axis=1, keepdims=True))
                weight = jnp.exp2((score - top) * factor)
                keep = jnp.exp2((old - top) * factor)
                lanes = sum(weight[:, i * HEAD_SIZE : (i + 1) * HEAD_SIZE] for i in range(span // HEAD_SIZE))
                l_ref[at, :] = l_ref[at, :] * keep + lanes
                acc_ref[at, :] = acc_ref[at, :] * keep + jnp.dot(
                    weight.astype(jnp.bfloat16), v, preferred_element_type=jnp.float32
                )
                m_ref[at, :] = jnp.broadcast_to(top, (pair_rows, HEAD_SIZE))
            return 0

        lax.fori_loop(first_ref[tile], back + 1, one_span, 0)
        for head in range(heads):
            at = pl.ds(head * TILE, TILE)
            total = jnp.sum(l_ref[at, :], axis=1, keepdims=True)
            o_ref[rows, head * HEAD_SIZE : (head + 1) * HEAD_SIZE] = (acc_ref[at, :] / total).astype(jnp.bfloat16)
        return 0

    lax.fori_loop(0, span // TILE, one_tile, 0)


def attend(first, low, q, own, ahead, behind):
    span, width = q.shape
    back, split, heads = len(ahead), ahead[0].shape[0], width // HEAD_SIZE
    vmem = pl.BlockSpec(memory_space=pltpu.VMEM)
    stat = pltpu.VMEM((heads * TILE, HEAD_SIZE), jnp.float32)
    return pl.pallas_call(
        functools.partial(attend_kernel, back=back, split=split, heads=heads),
        out_shape=jax.ShapeDtypeStruct((span, width), jnp.bfloat16),
        in_specs=[pl.BlockSpec(memory_space=pltpu.SMEM)] + [vmem] * (3 + 2 * back),
        out_specs=vmem,
        scratch_shapes=[pltpu.VMEM((back + 1,) + own.shape, jnp.bfloat16), stat, stat, stat],
        compiler_params=pltpu.CompilerParams(vmem_limit_bytes=32 * 1024 * 1024),
        name="attend",
    )(first, low, q, own, *ahead, *behind)


def local(queries, keys, values, doc_lengths):
    sp = lax.axis_size("sp")
    tokens = queries.shape[0]
    kv_heads = keys.shape[1] // HEAD_SIZE
    span = TEAM * tokens
    back = LONGEST // span
    split = span // 2
    teams = [list(range(i, i + TEAM)) for i in range(0, sp, TEAM)]

    def regroup(block):
        return lax.all_to_all(block, "sp", split_axis=1, concat_axis=0, axis_index_groups=teams, tiled=True)

    per_head = (tokens, kv_heads, 1, HEAD_SIZE)
    both = jnp.concatenate([keys.reshape(per_head), values.reshape(per_head)], axis=2)
    own = regroup(both.reshape(tokens, 2 * kv_heads * HEAD_SIZE))
    q = regroup(queries)

    ahead, behind = [], []
    up, down = own[:split], shift(own[split:], TEAM * (back + 1))
    for _ in range(back):
        up = shift(up, TEAM)
        down = shift(down, -TEAM)
        ahead.append(up)
        behind.append(down)
    behind = behind[::-1]

    range_index = lax.axis_index("tp") * lax.axis_size("dp") + lax.axis_index("dp")
    place = range_index * sp + lax.axis_index("sp")
    start = (place // TEAM) * span
    ends = jnp.cumsum(doc_lengths)
    where_at = start + jnp.arange(span, dtype=jnp.int32)
    low = jnp.max(jnp.where(ends[None, :] <= where_at[:, None], ends[None, :], 0), axis=1, keepdims=True)
    low = low - (start - back * span)
    first = low[::TILE, 0] // span

    out = attend(first, low, q, own, ahead, behind)
    return lax.all_to_all(out, "sp", split_axis=0, concat_axis=1, axis_index_groups=teams, tiled=True)


def solution(mesh):
    rows = P(("groups", "tp", "dp", "sp"), None)
    in_specs = (rows, rows, rows, P("groups"))
    return jax.shard_map(local, mesh=mesh, in_specs=in_specs, out_specs=rows, check_vma=False)
```

```python
import functools
import math

import jax
import jax.numpy as jnp
from jax import lax
from jax.experimental import pallas as pl
from jax.experimental.pallas import tpu as pltpu
from jax.sharding import PartitionSpec as P

HEAD_SIZE = 128
LONGEST = 2048
TEAM = 4
TILE = 128
DEAD = -1e30


def shift(block, distance):
    names = ("sp", "tp", "dp")
    sp, tp, dp = (lax.axis_size(name) for name in names)
    count = sp * tp * dp

    def flat(place):
        token_range, within = divmod(place % count, sp)
        return within * tp * dp + token_range

    route = [(flat(i), flat(i + distance)) for i in range(count)]
    return lax.ppermute(block, names, route)


def attend_kernel(first_ref, low_ref, q_ref, *refs, head_range, kv_head, keys_step, per, unroll):
    pieces, (o_ref, kv_ref, bias_ref) = refs[:-3], refs[-3:]
    span = q_ref.shape[0]
    total_keys = kv_ref.shape[0]
    first_head, heads = head_range
    half = pieces[0].shape[0]
    lanes = slice(kv_head * 2 * HEAD_SIZE, (kv_head + 1) * 2 * HEAD_SIZE)
    for i, piece in enumerate(pieces):
        kv_ref[i * half : (i + 1) * half] = piece[:, lanes]
    factor = HEAD_SIZE ** (-0.5) * math.log2(math.e)
    steps = total_keys // keys_step

    def one_tile(tile, _):
        rows = pl.ds(pl.multiple_of(tile * TILE, TILE), TILE)
        low = low_ref[rows, :]

        def with_steps(count):
            start = total_keys - count * keys_step
            shape = (TILE, count * keys_step)
            mine = total_keys - span + tile * TILE + lax.broadcasted_iota(jnp.int32, shape, 0)
            key = start + lax.broadcasted_iota(jnp.int32, shape, 1)
            bias_ref[:, start:] = jnp.where((key >= low) & (key <= mine), 0.0, DEAD)

            def head_lanes(head):
                return pl.ds(pl.multiple_of(head * HEAD_SIZE, HEAD_SIZE), HEAD_SIZE)

            def scores(batch):
                q = jnp.concatenate(
                    [q_ref[rows, head_lanes(first_head + batch * per + i)] for i in range(per)], axis=0
                )
                return lax.dot_general(
                    q, kv_ref[start:, :HEAD_SIZE], (((1,), (1,)), ((), ())), preferred_element_type=jnp.float32
                )

            def finish(batch, score):
                score = score + jnp.concatenate([bias_ref[:, start:]] * per, axis=0)
                top = jnp.max(score, axis=1, keepdims=True)
                weight = jnp.exp2((score - top) * factor)
                total = jnp.sum(weight, axis=1, keepdims=True)
                summed = jnp.dot(
                    weight.astype(jnp.bfloat16), kv_ref[start:, HEAD_SIZE:], preferred_element_type=jnp.float32
                )
                out = (summed / total).astype(jnp.bfloat16)
                for i in range(per):
                    o_ref[rows, head_lanes(batch * per + i)] = out[i * TILE : (i + 1) * TILE]

            def batches(index, _):
                coming = scores(index * unroll)
                for i in range(unroll):
                    score = coming
                    if i + 1 < unroll:
                        coming = scores(index * unroll + i + 1)
                    finish(index * unroll + i, score)
                return 0

            lax.fori_loop(0, heads // per // unroll, batches, 0)

        live = steps - first_ref[tile]
        for count in range(1, steps + 1):
            pl.when(live == count)(functools.partial(with_steps, count))
        return 0

    lax.fori_loop(0, span // TILE, one_tile, 0)


def attend(first, low, q, pieces, head_range, kv_head=0, keys_step=512, unroll=4):
    span = q.shape[0]
    width = head_range[1] * HEAD_SIZE
    total_keys = sum(piece.shape[0] for piece in pieces)
    vmem = pl.BlockSpec(memory_space=pltpu.VMEM)
    return pl.pallas_call(
        functools.partial(
            attend_kernel, head_range=head_range, kv_head=kv_head, keys_step=keys_step, per=2, unroll=unroll
        ),
        out_shape=jax.ShapeDtypeStruct((span, width), jnp.bfloat16),
        in_specs=[pl.BlockSpec(memory_space=pltpu.SMEM)] + [vmem] * (2 + len(pieces)),
        out_specs=vmem,
        scratch_shapes=[
            pltpu.VMEM((total_keys, 2 * HEAD_SIZE), jnp.bfloat16),
            pltpu.VMEM((TILE, total_keys), jnp.float32),
        ],
        compiler_params=pltpu.CompilerParams(vmem_limit_bytes=32 * 1024 * 1024),
        cost_estimate=pl.CostEstimate(flops=4 * span * width * total_keys, transcendentals=0, bytes_accessed=0),
        name="attend",
    )(first, low, q, *pieces)


def local(queries, keys, values, doc_lengths):
    sp = lax.axis_size("sp")
    tokens = queries.shape[0]
    kv_heads = keys.shape[1] // HEAD_SIZE
    span = TEAM * tokens
    half = span // 2
    back = LONGEST // span
    teams = [list(range(i, i + TEAM)) for i in range(0, sp, TEAM)]

    def regroup(block):
        return lax.all_to_all(block, "sp", split_axis=1, concat_axis=0, axis_index_groups=teams, tiled=True)

    per_head = (tokens, kv_heads, 1, HEAD_SIZE)
    both = jnp.concatenate([keys.reshape(per_head), values.reshape(per_head)], axis=2)
    own = regroup(both.reshape(tokens, 2 * kv_heads * HEAD_SIZE))
    q = regroup(queries)

    pieces = {(0, 0): own[:half], (0, 1): own[half:]}
    pieces[back, 1] = shift(pieces[0, 1], TEAM * back)
    pieces[1, 0] = shift(pieces[0, 0], TEAM)
    for step in range(1, back):
        pieces[back - step, 1] = shift(pieces[back - step + 1, 1], -TEAM)
        pieces[step + 1, 0] = shift(pieces[step, 0], TEAM)

    range_index = lax.axis_index("tp") * lax.axis_size("dp") + lax.axis_index("dp")
    place = range_index * sp + lax.axis_index("sp")
    start = (place // TEAM) * span
    ends = jnp.cumsum(doc_lengths)
    where_at = start + jnp.arange(span, dtype=jnp.int32)
    low = jnp.max(jnp.where(ends[None, :] <= where_at[:, None], ends[None, :], 0), axis=1, keepdims=True)
    low = low - (start - back * span)
    first = low[::TILE, 0] // 512
    ordered = [pieces[distance, which] for distance in range(back, -1, -1) for which in range(2)]
    out = attend(first, low, q, ordered, (0, q.shape[1] // HEAD_SIZE))
    return lax.all_to_all(out, "sp", split_axis=0, concat_axis=1, axis_index_groups=teams, tiled=True)


def solution(mesh):
    rows = P(("groups", "tp", "dp", "sp"), None)
    in_specs = (rows, rows, rows, P("groups"))
    return jax.shard_map(local, mesh=mesh, in_specs=in_specs, out_specs=rows, check_vma=False)
```

```python
import functools
import math

import jax
import jax.numpy as jnp
from jax import lax
from jax.experimental import pallas as pl
from jax.experimental.pallas import tpu as pltpu
from jax.sharding import PartitionSpec as P


HEAD_SIZE = 128
LONGEST = 2048
TEAM = 4
TILE = 128
DEAD = -1e30


def shift(block, distance):
    names = ("sp", "tp", "dp")
    sp, tp, dp = (lax.axis_size(name) for name in names)
    count = sp * tp * dp

    def flat(place):
        token_range, within = divmod(place % count, sp)
        return within * tp * dp + token_range

    route = [(flat(i), flat(i + distance)) for i in range(count)]
    return lax.ppermute(block, names, route)


def attend_kernel(low_first_ref, low_ref, q_ref, *refs, bases, starts, begin, per, unroll):
    pieces, refs = refs[: len(bases)], refs[len(bases) :]
    if begin:
        *state, kv_ref, bias_ref = refs
    else:
        *state, o_ref, kv_ref, bias_ref = refs
    top_ref, total_ref, sum_ref = state
    span = q_ref.shape[0]
    heads = q_ref.shape[1] // HEAD_SIZE
    window = LONGEST + span
    ats = [0]
    for piece in pieces:
        kv_ref[ats[-1] : ats[-1] + piece.shape[0]] = piece[...]
        ats.append(ats[-1] + piece.shape[0])
    total_keys = ats[-1]
    factor = HEAD_SIZE ** (-0.5) * math.log2(math.e)

    def one_tile(tile, _):
        rows = pl.ds(pl.multiple_of(tile * TILE, TILE), TILE)
        low = low_ref[rows, :]
        low_first = low_first_ref[tile]

        def head_lanes(head):
            return pl.ds(pl.multiple_of(head * HEAD_SIZE, HEAD_SIZE), HEAD_SIZE)

        def held(batch):
            return pl.ds(pl.multiple_of((tile * heads + batch * per) * TILE, TILE), per * TILE)

        def store(batch, out):
            for i in range(per):
                o_ref[rows, head_lanes(batch * per + i)] = out[i * TILE : (i + 1) * TILE].astype(jnp.bfloat16)

        def with_pieces(first_piece):
            start = ats[first_piece]
            shape = (TILE, total_keys - start)
            mine = window - span + tile * TILE + lax.broadcasted_iota(jnp.int32, shape, 0)
            at = start + lax.broadcasted_iota(jnp.int32, shape, 1)
            key = at + (bases[first_piece] - start)
            for i in range(first_piece + 1, len(bases)):
                gap = bases[i] - ats[i] - (bases[i - 1] - ats[i - 1])
                if gap:
                    key = key + jnp.where(at >= ats[i], gap, 0)
            bias_ref[:, start:] = jnp.where((key >= low) & (key <= mine), 0.0, DEAD)

            def scores(batch):
                q = jnp.concatenate([q_ref[rows, head_lanes(batch * per + i)] for i in range(per)], axis=0)
                return lax.dot_general(
                    q, kv_ref[start:, :HEAD_SIZE], (((1,), (1,)), ((), ())), preferred_element_type=jnp.float32
                )

            def finish(batch, score):
                score = score + jnp.concatenate([bias_ref[:, start:]] * per, axis=0)
                top = jnp.max(score, axis=1, keepdims=True)
                if not begin:
                    before = top_ref[held(batch), :]
                    top = jnp.maximum(top, before)
                    keep = jnp.exp2((before - top) * factor)
                    weight = jnp.exp2(
                        (score - jnp.concatenate([top] * (score.shape[1] // HEAD_SIZE), axis=1)) * factor
                    )
                else:
                    weight = jnp.exp2((score - top) * factor)
                total = jnp.sum(weight, axis=1, keepdims=True)
                summed = jnp.dot(
                    weight.astype(jnp.bfloat16), kv_ref[start:, HEAD_SIZE:], preferred_element_type=jnp.float32
                )
                if begin:
                    top_ref[held(batch), :] = jnp.broadcast_to(top, summed.shape)
                    total_ref[held(batch), :] = jnp.broadcast_to(total, summed.shape)
                    sum_ref[held(batch), :] = summed
                else:
                    total = total + total_ref[held(batch), :] * keep
                    store(batch, (summed + sum_ref[held(batch), :] * keep) / total)

            def batches(index, _):
                coming = scores(index * unroll)
                for i in range(unroll):
                    score = coming
                    if i + 1 < unroll:
                        coming = scores(index * unroll + i + 1)
                    finish(index * unroll + i, score)
                return 0

            lax.fori_loop(0, heads // per // unroll, batches, 0)

        def ends_before(piece):
            return bases[piece] + pieces[piece].shape[0] <= low_first

        for i, first_piece in enumerate(starts):
            live = jnp.bool_(True) if first_piece == 0 else ends_before(first_piece - 1)
            if i + 1 < len(starts):
                live = live & ~ends_before(starts[i + 1] - 1)
            elif not begin:
                live = live & ~ends_before(len(bases) - 1)
            pl.when(live)(functools.partial(with_pieces, first_piece))
        if not begin:

            @pl.when(ends_before(len(bases) - 1))
            def _():
                for batch in range(heads // per):
                    store(batch, sum_ref[held(batch), :] / total_ref[held(batch), :])

        return 0

    lax.fori_loop(0, span // TILE, one_tile, 0)


def attend(low_first, low, q, pieces, starts, state=None):
    span, width = q.shape
    bases, arrays = [base for base, _ in pieces], [array for _, array in pieces]
    total_keys = sum(array.shape[0] for array in arrays)
    begin = state is None
    vmem = pl.BlockSpec(memory_space=pltpu.VMEM)
    inputs = [low_first, low, q, *arrays] + ([] if begin else list(state))
    if begin:
        held = jax.ShapeDtypeStruct((span * width // HEAD_SIZE, HEAD_SIZE), jnp.float32)
        out_shape, out_specs = [held] * 3, [vmem] * 3
    else:
        out_shape, out_specs = jax.ShapeDtypeStruct(q.shape, jnp.bfloat16), vmem
    return pl.pallas_call(
        functools.partial(attend_kernel, bases=bases, starts=starts, begin=begin, per=2, unroll=4),
        out_shape=out_shape,
        in_specs=[pl.BlockSpec(memory_space=pltpu.SMEM)] + [vmem] * (len(inputs) - 1),
        out_specs=out_specs,
        scratch_shapes=[
            pltpu.VMEM((total_keys, 2 * HEAD_SIZE), jnp.bfloat16),
            pltpu.VMEM((TILE, total_keys), jnp.float32),
        ],
        compiler_params=pltpu.CompilerParams(vmem_limit_bytes=24 * 1024 * 1024),
        cost_estimate=pl.CostEstimate(flops=4 * q.size * total_keys, transcendentals=0, bytes_accessed=0),
    )(*inputs)


def local(queries, keys, values, doc_lengths):
    sp = lax.axis_size("sp")
    tokens = queries.shape[0]
    kv_heads = keys.shape[1] // HEAD_SIZE
    span = TEAM * tokens
    split = span * 12 // 16
    back = LONGEST // span
    teams = [list(range(i, i + TEAM)) for i in range(0, sp, TEAM)]

    def regroup(block):
        return lax.all_to_all(block, "sp", split_axis=1, concat_axis=0, axis_index_groups=teams, tiled=True)

    per_head = (tokens, kv_heads, 1, HEAD_SIZE)
    both = jnp.concatenate([keys.reshape(per_head), values.reshape(per_head)], axis=2)
    own = regroup(both.reshape(tokens, 2 * kv_heads * HEAD_SIZE))
    q = regroup(queries)

    pieces = {(0, 0): own[:split], (0, 1): own[split:]}
    down = shift(pieces[0, 1], TEAM * (back + 1))
    for step in range(1, back + 1):
        pieces[step, 0] = shift(pieces[step - 1, 0], TEAM)
        if step > 0:
            down = shift(down, -TEAM)
        pieces[back + 1 - step, 1] = down

    range_index = lax.axis_index("tp") * lax.axis_size("dp") + lax.axis_index("dp")
    place = range_index * sp + lax.axis_index("sp")
    start = (place // TEAM) * span
    ends = jnp.cumsum(doc_lengths)
    where_at = start + jnp.arange(span, dtype=jnp.int32)
    low = jnp.max(jnp.where(ends[None, :] <= where_at[:, None], ends[None, :], 0), axis=1, keepdims=True)
    low = low - (start - back * span)
    low_first = low[::TILE, 0]

    def in_order(chosen):
        chosen = sorted(chosen, key=lambda piece: (-piece[0], piece[1]))
        return [((back - distance) * span + part * split, pieces[distance, part]) for distance, part in chosen]

    late = [(back, 0)]
    early = [piece for piece in pieces if piece not in late]
    state = attend(low_first, low, q, in_order(early), (0, 1, 3, 5, 7))
    out = attend(low_first, low, q, in_order(late), (0,), state)
    return lax.all_to_all(out, "sp", split_axis=0, concat_axis=1, axis_index_groups=teams, tiled=True)


def solution(mesh):
    rows = P(("groups", "tp", "dp", "sp"), None)
    in_specs = (rows, rows, rows, P("groups"))

    return jax.shard_map(local, mesh=mesh, in_specs=in_specs, out_specs=rows, check_vma=False)
```
